32 devices in a mesh: fsdp: 4 (over y, core), tp: 4 (over z), rollout: 2 (over x).
Axes of the slice: x: 2, y: 2, z: 4, core: 2. Of those that a mesh axis runs over, the one named last changes fastest.
Arguments:
- weights: bfloat16 [2, 4096, 14336], P('rollout', 'fsdp', 'tp'), may hold values from -6 to 6
- gradient: bfloat16 [2, 4096, 14336], P('rollout', 'fsdp', 'tp'), may hold values from -6 to 6
- momentum: float32 [2, 4096, 14336], P('rollout', 'fsdp', 'tp'), may hold values from -90 to 90
- basis: float32 [2, 14336, 512], P('rollout', 'tp'), may hold values from -6 to 6
Outputs:
- weights_next: bfloat16 [2, 4096, 14336], P('rollout', 'fsdp', 'tp')
- momentum_next: float32 [2, 4096, 14336], P('rollout', 'fsdp', 'tp')
- basis_next: float32 [2, 14336, 512], P('rollout', 'tp')
- rollout_weights: bfloat16 [2, 4096, 14336], P(None, 'fsdp', 'tp')
The draws below stay inside these ranges and needn't reach their ends.
All inputs are finite; a program needn't handle non-finite values.
Results may differ from the reference program's by a relative error of at most 0.013.
Values may be sent and summed in bfloat16 or wider, within the bound.
A program may use at most 192 MiB of HBM per device.

```python
import math
import jax
import jax.numpy as jnp
from jax import lax

ROWS = 4096
COLS = 14336
RANK = 512


def draw_momentum(key, part):
    key_base = jax.random.fold_in(key, 11)
    key_cols = jax.random.fold_in(key, 12)
    key_rows = jax.random.fold_in(key, 13)
    base = jnp.clip(jax.random.normal(key_base, (2, ROWS, COLS), jnp.float32), -6.0, 6.0)
    top = 10.0
    rising = jnp.exp(math.log(3.0) * jnp.arange(COLS, dtype=jnp.float32) / COLS)
    column_scale = jnp.exp(jax.random.uniform(key_cols, (2, 1, COLS), jnp.float32, 0.0, math.log(top))) * rising
    row_scale = jnp.exp(jax.random.uniform(key_rows, (2, ROWS, 1), jnp.float32, 0.0, math.log(4.0)))
    return base * column_scale * row_scale / 8.0


def level_of(rng, shape, pieces, least, top_value):
    loudness = 1.0
    for dim, shards_of in pieces:
        heights = jax.random.uniform(jax.random.fold_in(jax.random.fold_in(rng, 6), dim), (shards_of,), jnp.float32, least / len(pieces), top_value / len(pieces))
        loudness = loudness * jnp.repeat(jnp.exp(heights), shape[dim] // shards_of).reshape((-1,) + (1,) * (len(shape) - 1 - dim))
    return loudness


def scatter_about(own_key, extent, width, most, shards=(), kind=jnp.bfloat16):
    values = width * jax.random.normal(own_key, extent, jnp.float32)
    if shards:
        values = values * level_of(own_key, extent, shards, -0.22, 0.18)
    return jnp.clip(values, -most, most).astype(kind)


def setup_inputs(seed: int = 0) -> dict:
    splits = jax.random.split(jax.random.key(seed), 5)
    weights = scatter_about(splits[0], (2, ROWS, COLS), 1.0, 6.0, ((0, 2), (1, 4), (2, 4)))
    gradient = scatter_about(splits[1], (2, ROWS, COLS), 1.0, 6.0, ((0, 2), (1, 4), (2, 4)))
    momentum = draw_momentum(jax.random.fold_in(splits[4], 71), 0)
    basis = scatter_about(splits[3], (2, COLS, RANK), 1.0, 6.0, ((0, 2), (1, 4)), jnp.float32)
    return dict(weights=weights, gradient=gradient, momentum=momentum, basis=basis)


HIGH = lax.Precision.HIGHEST

def one_matrix(weight, grad, moment, prior):
    blend = moment + grad.astype(jnp.float32)
    left = jnp.dot(blend.astype(jnp.float32), prior.astype(jnp.float32), precision=HIGH, preferred_element_type=jnp.float32)
    gram = jnp.dot(left.T.astype(jnp.float32), left.astype(jnp.float32), precision=HIGH, preferred_element_type=jnp.float32)
    lower = jnp.linalg.cholesky(gram)
    ortho = lax.linalg.triangular_solve(lower, left, left_side=False, lower=True, transpose_a=True)
    right = jnp.dot(blend.T.astype(jnp.float32), ortho.astype(jnp.float32), precision=HIGH, preferred_element_type=jnp.float32)
    meansq = lax.optimization_barrier(jnp.sum(right * right, axis=0)) / COLS
    basis_new = right * lax.rsqrt(meansq + 1e-06)
    moment_new = blend - 0.05 * jnp.dot(ortho.astype(jnp.float32), right.T.astype(jnp.float32), precision=HIGH, preferred_element_type=jnp.float32)
    update = jnp.dot(ortho.astype(jnp.float32), basis_new.T.astype(jnp.float32), precision=HIGH, preferred_element_type=jnp.float32)
    weight_new = (weight.astype(jnp.float32) - 0.3 * update).astype(jnp.bfloat16)
    return (weight_new, moment_new, basis_new)

def reference(weights, gradient, momentum, basis):
    first = one_matrix(weights[0], gradient[0], momentum[0], basis[0])
    second = one_matrix(weights[1], gradient[1], momentum[1], basis[1])
    weights_next = jnp.stack([first[0], second[0]])
    momentum_next = jnp.stack([first[1], second[1]])
    basis_next = jnp.stack([first[2], second[2]])
    return (weights_next, momentum_next, basis_next, weights_next)
```

```python
import functools

import jax
import jax.numpy as jnp
from jax import lax
from jax.experimental import pallas as pl
from jax.experimental.pallas import tpu as pltpu
from jax.sharding import PartitionSpec as P


HIGH = lax.Precision.HIGHEST
BLOCK = 128


def dot_t(a, b):
    return lax.dot_general(
        a, b, (((1,), (1,)), ((), ())), precision=HIGH, preferred_element_type=jnp.float32
    )


def factor_kernel(g_ref, x_ref, a_ref, w_ref, s_ref, v_ref):
    n = g_ref.shape[0]
    nb = BLOCK
    a_ref[...] = g_ref[...]
    w_ref[...] = jnp.where(
        lax.broadcasted_iota(jnp.int32, (n, n), 0) == lax.broadcasted_iota(jnp.int32, (n, n), 1),
        1.0,
        0.0,
    ).astype(jnp.float32)
    lane = lax.broadcasted_iota(jnp.int32, (nb, nb), 1)
    sub = lax.broadcasted_iota(jnp.int32, (nb, nb), 0)
    lane_row = lax.broadcasted_iota(jnp.int32, (1, nb), 1)
    sub_col = lax.broadcasted_iota(jnp.int32, (nb, 1), 0)

    def step(k, carry):
        s = s_ref[...]
        v = v_ref[...]
        row = s_ref[pl.ds(k, 1), :]
        vrow = v_ref[pl.ds(k, 1), :]
        p = jnp.sum(jnp.where(lane_row == k, row, 0.0), axis=1, keepdims=True)
        col = jnp.sum(jnp.where(lane == k, s, 0.0), axis=1, keepdims=True)
        col = jnp.where(sub_col > k, col, 0.0)
        rp = 1.0 / p
        r = lax.rsqrt(p)
        r = r * (1.5 - 0.5 * p * r * r)
        s_ref[...] = s - col * (row * rp)
        v_ref[...] = v - col * (vrow * rp)
        v_ref[pl.ds(k, 1), :] = vrow * r
        return carry

    for lo in range(0, n, nb):
        hi = lo + nb
        s_ref[...] = a_ref[lo:hi, lo:hi]
        v_ref[...] = jnp.where(lane == sub, 1.0, 0.0).astype(jnp.float32)
        lax.fori_loop(0, nb, step, 0)
        inv = v_ref[...]
        x = jnp.dot(inv, w_ref[lo:hi, :hi], precision=HIGH, preferred_element_type=jnp.float32)
        x_ref[lo:hi, :hi] = x
        if hi < n:
            x_ref[lo:hi, hi:] = jnp.zeros((nb, n - hi), jnp.float32)
            panel = dot_t(a_ref[hi:, lo:hi], inv)
            a_ref[hi:, hi:] = a_ref[hi:, hi:] - dot_t(panel, panel)
            w_ref[hi:, :hi] = w_ref[hi:, :hi] - jnp.dot(
                panel, x, precision=HIGH, preferred_element_type=jnp.float32
            )


def inverse_factor(gram):
    n = gram.shape[0]
    return pl.pallas_call(
        factor_kernel,
        out_shape=jax.ShapeDtypeStruct((n, n), jnp.float32),
        in_specs=[pl.BlockSpec(memory_space=pltpu.VMEM)],
        out_specs=pl.BlockSpec(memory_space=pltpu.VMEM),
        scratch_shapes=[
            pltpu.VMEM((n, n), jnp.float32),
            pltpu.VMEM((n, n), jnp.float32),
            pltpu.VMEM((BLOCK, BLOCK), jnp.float32),
            pltpu.VMEM((BLOCK, BLOCK), jnp.float32),
        ],
        compiler_params=pltpu.CompilerParams(vmem_limit_bytes=16 << 20),
        cost_estimate=pl.CostEstimate(flops=2_000_000_000, bytes_accessed=8 * n * n, transcendentals=0),
        name="factor",
    )(gram)


def updated(w_ref, ortho_ref, right_ref, inv_ref):
    base = (right_ref[...].astype(jnp.float32) * inv_ref[...]).astype(jnp.bfloat16)
    update = lax.dot_general(
        ortho_ref[...], base, (((1,), (1,)), ((), ())), preferred_element_type=jnp.float32
    )
    return (w_ref[0].astype(jnp.float32) - 0.3 * update).astype(jnp.bfloat16)


def own_kernel(who_ref, w_ref, ortho_ref, right_ref, inv_ref, new_ref, both_ref):
    value = updated(w_ref, ortho_ref, right_ref, inv_ref)
    new_ref[0] = value
    both_ref[0] = value


def other_kernel(who_ref, w_ref, ortho_ref, right_ref, inv_ref, both_in, both_ref):
    both_ref[0] = updated(w_ref, ortho_ref, right_ref, inv_ref)


def pick(n, sizes):
    for s in sizes:
        if n % s == 0:
            return s
    return n


def apply_update(who, w, ortho, right, inv, both=None):
    _, rows, cols = w.shape
    rank = ortho.shape[1]
    tr = pick(rows, (512, 256, 128))
    tc = pick(cols, (896, 512, 256, 128))
    w_spec = pl.BlockSpec((1, tr, tc), lambda j, i, who: (0, i, j))
    both_spec = pl.BlockSpec((1, tr, tc), lambda j, i, who: (who[0], i, j))
    in_specs = [
        w_spec,
        pl.BlockSpec((tr, rank), lambda j, i, who: (i, 0)),
        pl.BlockSpec((tc, rank), lambda j, i, who: (j, 0)),
        pl.BlockSpec((1, rank), lambda j, i, who: (0, 0)),
    ]
    both_shape = jax.ShapeDtypeStruct((2, rows, cols), jnp.bfloat16)
    args = [who, w, ortho, right, inv]
    if both is None:
        kernel = own_kernel
        out_shape = (jax.ShapeDtypeStruct((1, rows, cols), jnp.bfloat16), both_shape)
        out_specs = (w_spec, both_spec)
        aliases = {}
    else:
        kernel = other_kernel
        in_specs.append(pl.BlockSpec(memory_space=pl.ANY))
        args.append(both)
        out_shape = both_shape
        out_specs = both_spec
        aliases = {5: 0}
    return pl.pallas_call(
        kernel,
        out_shape=out_shape,
        grid_spec=pltpu.PrefetchScalarGridSpec(
            num_scalar_prefetch=1,
            grid=(cols // tc, rows // tr),
            in_specs=in_specs,
            out_specs=out_specs,
        ),
        input_output_aliases=aliases,
        compiler_params=pltpu.CompilerParams(vmem_limit_bytes=32 << 20),
        cost_estimate=pl.CostEstimate(
            flops=2 * rows * cols * rank, bytes_accessed=6 * rows * cols, transcendentals=0
        ),
        name="apply_own" if both is None else "apply_other",
    )(*args)


def body(weights, gradient, momentum, basis):
    swap = functools.partial(lax.ppermute, axis_name="rollout", perm=[(0, 1), (1, 0)])
    me = lax.axis_index("rollout")
    cols = weights.shape[2] * lax.axis_size("tp")
    weights_other = swap(weights)
    blend = momentum[0] + gradient[0].astype(jnp.float32)
    share = lax.psum_scatter(
        jnp.dot(blend, basis[0], precision=lax.Precision.HIGH, preferred_element_type=jnp.float32),
        "tp",
        scatter_dimension=0,
        tiled=True,
    )
    gram = lax.psum(
        jnp.dot(share.T, share, precision=HIGH, preferred_element_type=jnp.float32), ("fsdp", "tp")
    )
    share, gram = lax.optimization_barrier((share, gram))
    left = lax.all_gather(share, "tp", axis=0, tiled=True)
    inverse = inverse_factor(gram)
    ortho = dot_t(left, inverse).astype(jnp.bfloat16)
    ortho_other = swap(ortho)
    partial_right = lax.dot_general(
        blend.astype(jnp.bfloat16),
        ortho,
        (((0,), (0,)), ((), ())),
        preferred_element_type=jnp.float32,
    )
    right = lax.psum(partial_right.astype(jnp.bfloat16), "fsdp")
    right_other = swap(right)
    wide = right.astype(jnp.float32)
    squares = lax.psum(jnp.sum(wide * wide, axis=0, keepdims=True), "tp")
    inv = lax.rsqrt(squares / cols + 1e-06)
    inv_other = swap(inv)
    weight_new, both = apply_update(me.reshape(1), weights, ortho, right, inv)
    moment_new = blend - 0.05 * lax.dot_general(
        ortho, right, (((1,), (1,)), ((), ())), preferred_element_type=jnp.float32
    )
    basis_new = wide * inv
    both = apply_update((1 - me).reshape(1), weights_other, ortho_other, right_other, inv_other, both)
    return (weight_new, moment_new[None], basis_new[None], both)


def solution(mesh):
    return jax.shard_map(
        body,
        mesh=mesh,
        in_specs=(
            P("rollout", "fsdp", "tp"),
            P("rollout", "fsdp", "tp"),
            P("rollout", "fsdp", "tp"),
            P("rollout", "tp", None),
        ),
        out_specs=(
            P("rollout", "fsdp", "tp"),
            P("rollout", "fsdp", "tp"),
            P("rollout", "tp", None),
            P(None, "fsdp", "tp"),
        ),
        check_vma=False,
    )
```
